32 devices in a mesh: stream: 4 (over z), patch: 8 (over y, x, core).
Axes of the slice: x: 2, y: 2, z: 4, core: 2. Of those that a mesh axis runs over, the one named last changes fastest.
Arguments:
- tokens: bfloat16 [4, 1024, 1536], P('stream', 'patch'), may hold values from -6 to 6
- query_weight: bfloat16 [1536, 768], P('stream'), may hold values from -0.25 to 0.25
- key_weight: bfloat16 [1536, 768], P('stream'), may hold values from -0.25 to 0.25
- value_weight: bfloat16 [1536, 768], P('stream'), may hold values from -0.15625 to 0.15625
- cache_keys: bfloat16 [4, 6144, 768], P('stream', 'patch'), may hold values from -240 to 240, as said below
- cache_values: bfloat16 [4, 6144, 768], P('stream', 'patch'), may hold values from -6 to 6
- lengths: int32 [4, 8], P('stream', 'patch'), may hold values from 1 to 6, as said below
- assign: int32 [4, 256, 1], P('stream', 'patch'), may hold values from 0 to 7; in each aligned block of 32 rows (0 to 31, 32 to 63, ..., all dimensions but the last counted through in order) at most 8 rows name the same one
Outputs:
- attended: bfloat16 [4, 1024, 768], P('stream', 'patch')
- new_keys: bfloat16 [4, 2048, 768], P('stream', 'patch')
- new_values: bfloat16 [4, 2048, 768], P('stream', 'patch')
The draws below stay inside these ranges and needn't reach their ends.
Inputs may be any that keep to these rules, and one draw needn't show every extreme that they name: `lengths`: each stream's owners hold whole cache blocks of 128 tokens; in every stream exactly two owners hold 6 blocks and every other owner 1 or 2. `assign`: among the 32 groups of one device no owner is named more than 8 times. `cache_keys`: rows past an owner's length are not part of its cache.
All inputs are finite; a program needn't handle non-finite values.
Results may differ from the reference program's by a relative error of at most 0.015.
The reference program's roundings to bfloat16 on the way (of `normed` and `weights`) count: a program that leaves them out, or rounds other values in their place, can miss the bound.
Values may be sent and summed in bfloat16 or wider, within the bound.
No kernel may reach another device: no remote copies, remote signals or barrier semaphores. Data moves between devices by JAX's collectives and lax.ppermute only.
A program may use at most 128 MiB of HBM per device.

```python
import math
import jax
import jax.numpy as jnp
import numpy as np
from jax import lax

D = 1536
HEADS = 6
HD = 128
BLOCK = 128
CAP_BLK = 6
APP = 4
GROUPS = 4
OWNERS = 8
SPAN = 1024
NBD = 32
MOST = 8
SLOTS = 256


def stream_order(order_key):
    return jax.random.permutation(order_key, OWNERS)


def draw_lengths(key, part):
    base_key = jax.random.fold_in(key, 101)
    order_key = jax.random.fold_in(key, 102)
    base_len = jax.random.randint(base_key, (GROUPS, OWNERS), 1, 3)
    orders = jax.vmap(stream_order)(jax.random.split(order_key, GROUPS))
    return jnp.where(orders < 2, CAP_BLK, base_len).astype(jnp.int32)


def draw_cache_keys(key, part):
    full_shape = (GROUPS, OWNERS * CAP_BLK * BLOCK, HEADS * HD)
    drawn = jnp.clip(jax.random.normal(jax.random.fold_in(key, 203), full_shape, jnp.float32), -5.0, 5.0)
    return (drawn * 1.7).astype(jnp.bfloat16)


def block_levels(stream_key, shape, cuts, smallest, top_value):
    level, own = 1.0, jax.random.fold_in(stream_key, 6)
    for dim, shards_of in cuts:
        steps = jnp.exp(jax.random.uniform(jax.random.fold_in(own, dim), (shards_of,), jnp.float32, smallest / len(cuts), top_value / len(cuts)))
        level = level * jnp.repeat(steps, shape[dim] // shards_of).reshape([-1 if axis == dim else 1 for axis in range(len(shape))])
    return level


def assign_block(own_key, own, number, rows, count, top, most, lean):
    sequence = jax.random.permutation(own_key, count)
    heavy_load, ordinary = shares(count, rows * top, most, lean, True), shares(count, rows * top, most, lean, False)
    places = jnp.arange(count)

    def named(sizes, rotation):
        used = int((sizes > 0).sum())
        fixed = max(1, used // 4)
        shifted = fixed + (places - fixed + rotation * (used - fixed)) % max(1, count - fixed)
        return jnp.zeros((count,), jnp.int32).at[sequence[jnp.where(places < fixed, places, shifted)]].set(jnp.asarray(sizes, jnp.int32))

    sizes = jnp.where(number % 4 == 0, named(heavy_load, number // 4), named(ordinary, number - number // 4 - 1))
    mixed = jax.random.permutation(jax.random.fold_in(own, 3), count)
    source_of, receiver = mixed[0:count // 2 * 2:2], mixed[1:count // 2 * 2:2]
    room = jnp.minimum(sizes[source_of] - 1, most - sizes[receiver]) // 2
    room = jnp.where((source_of == sequence[0]) | (receiver == sequence[0]) | (sizes[receiver] == 0), 0, jnp.maximum(room, 0))
    shifted = jax.random.randint(jax.random.fold_in(own, 4), (count // 2,), 0, 1 << 20) % (room + 1)
    sizes = sizes.at[source_of].add(-shifted).at[receiver].add(shifted)
    labels = jnp.searchsorted(jnp.cumsum(sizes), jnp.arange(rows * top), side="right").astype(jnp.int32)
    grid = labels.reshape(top, rows).T
    grid = grid[jax.random.permutation(jax.random.fold_in(own, 1), rows)]
    rotation = jax.random.randint(jax.random.fold_in(own, 2), (rows, 1), 0, top)
    return jnp.take_along_axis(grid, (jnp.arange(top)[None, :] + rotation) % top, axis=1)


def shares(amount, total, most, slope, full):
    portions = [(1 << 20) // math.isqrt(grade ** slope) + 1 for grade in range(1, amount + 1)]
    largest = most if full else min(most, max(-(-total // amount), total * portions[0] // sum(portions)))
    least = 1 if total - largest >= amount - 1 else 0
    counts, spare = [largest] + [least] * (amount - 1), total - largest - least * (amount - 1)
    while spare > 0:
        free = [i for i in range(1, amount) if counts[i] < largest] or [i for i in range(1, amount) if counts[i] < most]
        mass, remaining = sum([portions[i] for i in free]), spare
        for i in free:
            more = min(most - counts[i], max(1, remaining * portions[i] // mass), spare)
            counts[i] = counts[i] + more
            spare = spare - more
    return np.array(counts)


def centred(key, dims, deviation, reach, shards=(), kind=jnp.bfloat16):
    array = deviation * jax.random.normal(key, dims, jnp.float32)
    if shards:
        array = array * block_levels(key, dims, shards, -0.22, 0.18)
    return jnp.clip(array, -reach, reach).astype(kind)


def setup_inputs(seed: int = 0) -> dict:
    seeds = jax.random.split(jax.random.key(seed), 9)
    tokens = centred(seeds[0], (GROUPS, SPAN, D), 1.0, 6.0, ((0, 4), (1, 8)))
    query_weight = centred(seeds[1], (D, HEADS * HD), (D // 3) ** -0.5, 0.25, ((0, 4),))
    key_weight = centred(seeds[2], (D, HEADS * HD), (D // 3) ** -0.5, 0.25, ((0, 4),))
    value_weight = centred(seeds[3], (D, HEADS * HD), D ** -0.5, 0.15625, ((0, 4),))
    cache_keys = draw_cache_keys(jax.random.fold_in(seeds[8], 71), 0)
    cache_values = centred(seeds[5], (GROUPS, OWNERS * CAP_BLK * BLOCK, HEADS * HD), 1.0, 6.0, ((0, 4), (1, 8)))
    lengths = draw_lengths(jax.random.fold_in(seeds[8], 71), 0)
    assign_keys = jax.random.split(jax.random.fold_in(seeds[7], 1), GROUPS * (OWNERS * NBD) // NBD)
    assign_turns = jax.random.permutation(jax.random.fold_in(seeds[7], 3), GROUPS * (OWNERS * NBD) // NBD)
    assign = jax.vmap(lambda own, number: assign_block(jax.random.fold_in(seeds[7], 2), own, number, NBD, OWNERS, 1, MOST, 2))(assign_keys, assign_turns).reshape((GROUPS, OWNERS * NBD, 1))
    return dict(tokens=tokens, query_weight=query_weight, key_weight=key_weight, value_weight=value_weight, cache_keys=cache_keys, cache_values=cache_values, lengths=lengths, assign=assign)


epsilon = 1e-06
masked_score = -1e+30

def normalize(rows):
    floats = rows.astype(jnp.float32)
    scaled = floats * lax.rsqrt(lax.optimization_barrier(jnp.mean(floats * floats, axis=-1, keepdims=True)) + epsilon)
    return scaled.astype(jnp.bfloat16)

def project(normed, weight):
    return jnp.dot(normed, weight, preferred_element_type=jnp.float32).astype(jnp.bfloat16)

def slot_table(owner_ids):
    positions = jnp.arange(NBD, dtype=jnp.int32)
    earlier = positions[None, :] < positions[:, None]
    matches = owner_ids[:, :, None] == owner_ids[:, None, :]
    ranks = lax.optimization_barrier(jnp.sum(jnp.logical_and(matches, earlier[None]).astype(jnp.int32), axis=2))
    targets = owner_ids * MOST + ranks
    slot_ids = jnp.arange(OWNERS * MOST, dtype=jnp.int32)
    return (targets[:, None, :] == slot_ids[None, :, None]).astype(jnp.float32)

def place_rows(select, rows):
    width = rows.shape[1]
    grouped = rows.reshape(OWNERS, NBD, APP * width).astype(jnp.float32)
    placed = jnp.einsum('psg,pgw->psw', select, grouped)
    placed = placed.reshape(OWNERS, OWNERS, MOST, APP * width).transpose(1, 0, 2, 3)
    return placed.reshape(OWNERS, SLOTS, width).astype(jnp.bfloat16)

def row_flags(select):
    filled = lax.optimization_barrier(jnp.sum(select, axis=2)).reshape(OWNERS, OWNERS, MOST).transpose(1, 0, 2)
    return jnp.repeat(filled.reshape(OWNERS, OWNERS * MOST), APP, axis=1)

def merge_block(state, query_f, keys_b, vals_b, live):
    best, numer, total = state
    key_rows = keys_b.reshape(-1, HEADS, HD).astype(jnp.float32)
    value_rows = vals_b.reshape(-1, HEADS, HD).astype(jnp.float32)
    scores = jnp.einsum('thd,khd->thk', query_f, key_rows) * (1.0 / math.sqrt(HD))
    scores = jnp.where(live[None, None, :], scores, masked_score)
    top_row = lax.optimization_barrier(jnp.max(scores, axis=2))
    weights = jnp.where(live[None, None, :], jnp.exp(scores - top_row[:, :, None]), 0.0).astype(jnp.bfloat16)
    part_numer = jnp.einsum('thk,khd->thd', weights.astype(jnp.float32), value_rows)
    part_total = lax.optimization_barrier(jnp.sum(weights.astype(jnp.float32), axis=2))
    merged = jnp.maximum(best, top_row)
    old_scale = jnp.exp(best - merged)
    new_scale = jnp.exp(top_row - merged)
    numer = numer * old_scale[:, :, None] + part_numer * new_scale[:, :, None]
    total = total * old_scale + part_total * new_scale
    return (merged, numer, total)

def attend(queries, cache_k, cache_v, owner_len, app_k, app_v, app_valid):
    query_f = queries.reshape(SPAN, HEADS, HD).astype(jnp.float32)
    block_ids = jnp.arange(CAP_BLK, dtype=jnp.int32)

    def visit(carry, owner):
        keys_o, vals_o, length_o, extra_k, extra_v, extra_valid = owner
        carry = merge_block(carry, query_f, extra_k, extra_v, extra_valid > 0.5)
        keys_blocks = keys_o.reshape(CAP_BLK, BLOCK, HEADS * HD)
        vals_blocks = vals_o.reshape(CAP_BLK, BLOCK, HEADS * HD)

        def per_block(inner, item):
            keys_b, vals_b, block_id = item
            live = jnp.full((BLOCK,), block_id < length_o)
            return (merge_block(inner, query_f, keys_b, vals_b, live), None)
        carry, _ = lax.scan(per_block, carry, (keys_blocks, vals_blocks, block_ids))
        return (carry, None)
    start_state = (jnp.full((SPAN, HEADS), masked_score, jnp.float32), jnp.zeros((SPAN, HEADS, HD), jnp.float32), jnp.zeros((SPAN, HEADS), jnp.float32))
    final_state, _ = lax.scan(visit, start_state, (cache_k, cache_v, owner_len, app_k, app_v, app_valid))
    numer = final_state[1]
    total = final_state[2]
    return (numer / total[:, :, None]).reshape(SPAN, HEADS * HD).astype(jnp.bfloat16)

def reference(tokens, query_weight, key_weight, value_weight, cache_keys, cache_values, lengths, assign):
    attended_list = []
    key_list = []
    value_list = []
    for stream_id in range(GROUPS):
        normed = normalize(tokens[stream_id])
        queries = project(normed, query_weight)
        keys_new = project(normed, key_weight)
        values_new = project(normed, value_weight)
        select = slot_table(assign[stream_id, :, 0].reshape(OWNERS, NBD).astype(jnp.int32))
        app_k = place_rows(select, keys_new)
        app_v = place_rows(select, values_new)
        app_valid = row_flags(select)
        cache_k = cache_keys[stream_id].reshape(OWNERS, CAP_BLK * BLOCK, HEADS * HD)
        cache_v = cache_values[stream_id].reshape(OWNERS, CAP_BLK * BLOCK, HEADS * HD)
        attended_list.append(attend(queries, cache_k, cache_v, lengths[stream_id], app_k, app_v, app_valid))
        key_list.append(app_k.reshape(OWNERS * SLOTS, HEADS * HD))
        value_list.append(app_v.reshape(OWNERS * SLOTS, HEADS * HD))
    return (jnp.stack(attended_list), jnp.stack(key_list), jnp.stack(value_list))
```

```python
import functools
import math

import jax
import jax.numpy as jnp
from jax import lax
from jax.experimental import pallas as pl
from jax.experimental.pallas import tpu as pltpu
from jax.sharding import PartitionSpec as P

HEADS = 6
HD = 128
BLOCK = 128
APP = 4
EPS = 1e-06
MASKED = -1e30
WIDTH = HEADS * HD
EXP_SCALE = math.log2(math.e) / math.sqrt(HD)
STAT_ROWS = 32


VMEM = pl.BlockSpec(memory_space=pltpu.VMEM)
SMEM = pl.BlockSpec(memory_space=pltpu.SMEM)
NT = (((1,), (1,)), ((), ()))
TN = (((0,), (0,)), ((), ()))


def call(kernel, out_shape, args, smem=0, scratch=(), flops=0, limit=60 * 1024 * 1024, name=None):
    return pl.pallas_call(
        kernel,
        out_shape=out_shape,
        in_specs=[SMEM] * smem + [VMEM] * (len(args) - smem),
        out_specs=jax.tree.map(lambda _: VMEM, out_shape),
        scratch_shapes=scratch,
        compiler_params=pltpu.CompilerParams(vmem_limit_bytes=limit),
        cost_estimate=pl.CostEstimate(flops=flops, bytes_accessed=1 << 20, transcendentals=0),
        name=name,
    )(*args)


def prepare_kernel(owners, most, me_ref, assign_ref, wq_ref, wk_ref, wv_ref, wt_ref, tgt_ref):
    me = me_ref[0]
    share = wt_ref.shape[0] // 3
    row = lax.broadcasted_iota(jnp.int32, (share, WIDTH), 0)
    col = lax.broadcasted_iota(jnp.int32, (share, WIDTH), 1)
    pick = (col == row + me * share).astype(jnp.float32).astype(jnp.bfloat16)
    for i, w_ref in enumerate((wq_ref, wk_ref, wv_ref)):
        part = lax.dot_general(pick, w_ref[...], NT, preferred_element_type=jnp.float32)
        wt_ref[i * share : (i + 1) * share, :] = part.astype(jnp.bfloat16)
    groups = assign_ref.shape[0]
    lanes = lax.broadcasted_iota(jnp.int32, (groups, 128), 1)
    owner = assign_ref[...]
    named = (lanes == owner).astype(jnp.float32)
    r = lax.broadcasted_iota(jnp.int32, (groups, groups), 0)
    c = lax.broadcasted_iota(jnp.int32, (groups, groups), 1)
    before = (c < r).astype(jnp.float32)
    seen = jnp.dot(before, named, preferred_element_type=jnp.float32)
    rank = jnp.sum(seen * named, axis=1, keepdims=True).astype(jnp.int32)
    base = (owner * owners + me) * (most * APP) + rank * APP
    token = lax.broadcasted_iota(jnp.int32, (groups, groups * APP), 1)
    group = lax.broadcasted_iota(jnp.int32, (groups, groups * APP), 0)
    mine = jnp.logical_and(token >= group * APP, token < group * APP + APP)
    spread = jnp.where(mine, base + token - group * APP, 0)
    tgt_ref[...] = jnp.broadcast_to(jnp.sum(spread, axis=0, keepdims=True), tgt_ref.shape)


def project_kernel(owners, shards, slots, ids_ref, *refs):
    me, zed = ids_ref[0], ids_ref[1]
    x_refs = refs[:owners]
    t_refs = refs[owners : 2 * owners]
    w_refs = refs[2 * owners : 2 * owners + shards]
    q_ref = refs[2 * owners + shards]
    kv_refs = refs[2 * owners + shards + 1 : 3 * owners + shards + 1]
    valid_ref, x_scr, t_scr, kv_scr = refs[3 * owners + shards + 1 :]
    rows = x_refs[0].shape[0]
    share = q_ref.shape[0]
    depth = w_refs[0].shape[1]
    for r in range(owners):
        src = jnp.bitwise_xor(me, r)
        floats = x_refs[r][...].astype(jnp.float32)
        mean = jnp.mean(floats * floats, axis=1, keepdims=True)
        normed = (floats * lax.rsqrt(mean + EPS)).astype(jnp.bfloat16)
        x_scr[pl.ds(pl.multiple_of(src * rows, rows), rows), :] = normed
        t_scr[:, pl.ds(pl.multiple_of(src * rows, rows), rows)] = t_refs[r][...]
    total = None
    for s in range(shards):
        at = pl.multiple_of(jnp.bitwise_xor(zed, s) * depth, depth)
        part = lax.dot_general(
            w_refs[s][...], x_scr[:, pl.ds(at, depth)], NT, preferred_element_type=jnp.float32
        )
        total = part if total is None else total + part
    q_ref[...] = total[:share].astype(jnp.bfloat16)
    kv_scr[...] = total[share:].astype(jnp.bfloat16)
    tokens = owners * rows
    targets = t_scr[0:1, :]
    slot = lax.broadcasted_iota(jnp.int32, (slots, tokens), 0)
    for r in range(owners):
        first = jnp.bitwise_xor(me, r) * slots
        hit = (slot == targets - first).astype(jnp.float32)
        if r == 0:
            valid_ref[...] = jnp.broadcast_to(
                jnp.sum(hit, axis=1, keepdims=True), valid_ref.shape
            )
        got = lax.dot_general(
            kv_scr[...], hit.astype(jnp.bfloat16), NT, preferred_element_type=jnp.float32
        )
        kv_refs[r][0] = got[:share].astype(jnp.bfloat16)
        kv_refs[r][1] = got[share:].astype(jnp.bfloat16)


def cached_kernel(count, tile, ids_ref, len_ref, *refs):
    q_refs = refs[:count]
    k_ref, v_ref, q_all, acc_ref, top_ref, total_ref = refs[count:]
    me = ids_ref[0]
    if count == 1:
        q_all[...] = q_refs[0][...]
    else:
        share = q_refs[0].shape[0]
        for r in range(count):
            at = pl.multiple_of(jnp.bitwise_xor(me, r) * share, share)
            q_all[pl.ds(at, share), :] = q_refs[r][...]
    tokens = q_all.shape[1]
    length = len_ref[0]
    capacity = k_ref.shape[0]

    def run(keys, masked):
        def head(h, carry):
            at = pl.multiple_of(h * HD, HD)
            key = k_ref[0:keys, pl.ds(at, HD)]
            value = v_ref[0:keys, pl.ds(at, HD)]

            def one(j):
                q = q_all[pl.ds(at, HD), pl.ds(j, tile)]
                s = jnp.dot(key, q, preferred_element_type=jnp.float32)
                if masked:
                    pos = lax.broadcasted_iota(jnp.int32, s.shape, 0)
                    s = jnp.where(pos < length * BLOCK, s, MASKED)
                top = jnp.max(s, axis=0, keepdims=True)
                w = jnp.exp2((s - top) * EXP_SCALE).astype(jnp.bfloat16)
                acc_ref[pl.ds(at, HD), pl.ds(j, tile)] = lax.dot_general(
                    value, w, TN, preferred_element_type=jnp.float32
                )
                total = jnp.sum(w.astype(jnp.float32), axis=0, keepdims=True)
                top_ref[pl.ds(pl.multiple_of(h * 8, 8), 8), pl.ds(j, tile)] = jnp.broadcast_to(
                    top, (8, tile)
                )
                total_ref[pl.ds(pl.multiple_of(h * 8, 8), 8), pl.ds(j, tile)] = jnp.broadcast_to(
                    total, (8, tile)
                )

            if tokens // tile <= 2:
                for j in range(tokens // tile):
                    one(j * tile)
            else:
                lax.fori_loop(
                    0,
                    tokens // tile,
                    lambda j, c: (one(pl.multiple_of(j * tile, tile)), c)[1],
                    0,
                )
            return carry

        lax.fori_loop(0, HEADS, head, 0)

    short = min(2 * BLOCK, capacity)

    @pl.when(length * BLOCK <= short)
    def _():
        run(short, True)

    if capacity > short:

        @pl.when(jnp.logical_and(length * BLOCK > short, length * BLOCK < capacity))
        def _():
            run(capacity, True)

        @pl.when(jnp.logical_and(length * BLOCK > short, length * BLOCK >= capacity))
        def _():
            run(capacity, False)


def appended_kernel(count, owners, tile, ids_ref, *refs):
    kv_refs = refs[:count]
    valid_ref, q_ref, acc_ref, top_ref, total_ref = refs[count : count + 5]
    nk_ref, nv_ref = refs[count + 5 : count + 7]
    out_refs = refs[count + 7 : count + 7 + owners]
    kt_scr, vt_scr, out_scr, stat_scr = refs[count + 7 + owners :]
    me = ids_ref[0]
    if count == 1:
        kt_scr[...] = kv_refs[0][0]
        vt_scr[...] = kv_refs[0][1]
    else:
        share = kv_refs[0].shape[1]
        for r in range(count):
            at = pl.multiple_of(jnp.bitwise_xor(me, r) * share, share)
            kt_scr[pl.ds(at, share), :] = kv_refs[r][0]
            vt_scr[pl.ds(at, share), :] = kv_refs[r][1]
    nk_ref[...] = kt_scr[...].astype(jnp.float32).T.astype(jnp.bfloat16)
    nv_ref[...] = vt_scr[...].astype(jnp.float32).T.astype(jnp.bfloat16)
    bias = jnp.where(valid_ref[:, 0:1] > 0.5, 0.0, MASKED)
    tokens = q_ref.shape[1]
    stat_scr[...] = jnp.zeros_like(stat_scr)

    def one(h, j):
        lo, hi = h * HD, (h + 1) * HD
        q = q_ref[lo:hi, pl.ds(j, tile)]
        s = jnp.dot(nk_ref[:, lo:hi], q, preferred_element_type=jnp.float32) + bias
        old_top = top_ref[8 * h : 8 * h + 1, pl.ds(j, tile)]
        top = jnp.maximum(jnp.max(s, axis=0, keepdims=True), old_top)
        w = jnp.exp2((s - top) * EXP_SCALE).astype(jnp.bfloat16)
        numer = jnp.dot(vt_scr[lo:hi, :], w, preferred_element_type=jnp.float32)
        old = jnp.exp2((old_top - top) * EXP_SCALE)
        total = (
            jnp.sum(w.astype(jnp.float32), axis=0, keepdims=True)
            + total_ref[8 * h : 8 * h + 1, pl.ds(j, tile)] * old
        )
        inverse = 1.0 / total
        mixed = acc_ref[lo:hi, pl.ds(j, tile)] * (old * inverse) + numer * inverse
        out_scr[lo:hi, pl.ds(j, tile)] = mixed.astype(jnp.bfloat16)
        level = top * EXP_SCALE + jnp.log2(total)
        high = level.astype(jnp.bfloat16).astype(jnp.float32)
        middle = (level - high).astype(jnp.bfloat16).astype(jnp.float32)
        stat_scr[h : h + 1, pl.ds(j, tile)] = high
        stat_scr[8 + h : 9 + h, pl.ds(j, tile)] = middle
        stat_scr[16 + h : 17 + h, pl.ds(j, tile)] = level - high - middle

    for h in range(HEADS):
        if tokens // tile <= 2:
            for j in range(tokens // tile):
                one(h, j * tile)
        else:
            lax.fori_loop(
                0,
                tokens // tile,
                lambda j, c, h=h: (one(h, pl.multiple_of(j * tile, tile)), c)[1],
                0,
            )
    rows = tokens // owners
    for r in range(owners):
        at = pl.multiple_of(jnp.bitwise_xor(me, r) * rows, rows)
        out_refs[r][0:WIDTH, :] = out_scr[:, pl.ds(at, rows)]
        out_refs[r][WIDTH:, :] = stat_scr[:, pl.ds(at, rows)].astype(jnp.bfloat16)


def finish_kernel(owners, *refs):
    got, out_ref = refs[:owners], refs[owners]
    levels = []
    for r in range(owners):
        stat = got[r][WIDTH:, :].astype(jnp.float32)
        levels.append(stat[0:8] + stat[8:16] + stat[16:24])
    best = functools.reduce(jnp.maximum, levels)
    factors = [jnp.exp2(level - best) for level in levels]
    inverse = 1.0 / functools.reduce(jnp.add, factors)
    factors = [factor * inverse for factor in factors]
    for h in range(HEADS):
        lo, hi = h * HD, (h + 1) * HD
        mixed = None
        for r in range(owners):
            part = got[r][lo:hi, :].astype(jnp.float32) * factors[r][h : h + 1, :]
            mixed = part if mixed is None else mixed + part
        out_ref[:, lo:hi] = mixed.T.astype(jnp.bfloat16)


def body(tokens, query_weight, key_weight, value_weight, cache_keys, cache_values, lengths, assign):
    owners = lax.axis_size("patch")
    shards = lax.axis_size("stream")
    rows = tokens.shape[1]
    groups = rows // APP
    most = max(2, 2 * groups // owners)
    slots = owners * most * APP
    share = WIDTH // owners
    span = owners * rows
    depth = query_weight.shape[0]
    me = lax.axis_index("patch").astype(jnp.int32)
    zed = lax.axis_index("stream").astype(jnp.int32)
    ids = jnp.stack((me, zed))
    bf16 = jnp.bfloat16

    def shape(*dims, dtype=bf16):
        return jax.ShapeDtypeStruct(dims, dtype)

    def swap(x, axis, r):
        size = lax.axis_size(axis)
        return lax.ppermute(x, axis, [(i, i ^ r) for i in range(size)])

    def spread(x):
        got = {0: x}
        for r in sorted(range(2, owners, 2), key=lambda r: (-bin(r).count("1"), r)):
            got[r] = swap(x, "patch", r)
        for r in range(0, owners, 2):
            got[r + 1] = swap(got[r], "patch", 1)
        return [got[r] for r in range(owners)]

    x_all = spread(tokens[0])
    wt, tgt = call(
        functools.partial(prepare_kernel, owners, most),
        (shape(3 * share, depth), shape(8, rows, dtype=jnp.int32)),
        (ids, assign[0], query_weight, key_weight, value_weight),
        smem=1,
        flops=6 * share * WIDTH * depth,
        name="prepare",
    )
    w_all = [wt] + [swap(wt, "stream", s) for s in range(1, shards)]
    t_all = spread(tgt)
    projected = call(
        functools.partial(project_kernel, owners, shards, slots),
        (
            (shape(share, span),)
            + (shape(2, share, slots),) * owners
            + (shape(slots, 128, dtype=jnp.float32),)
        ),
        (ids, *x_all, *t_all, *w_all),
        smem=1,
        scratch=[
            pltpu.VMEM((span, shards * depth), bf16),
            pltpu.VMEM((8, span), jnp.int32),
            pltpu.VMEM((2 * share, span), bf16),
        ],
        flops=6 * share * span * shards * depth,
        name="project",
    )
    q_own, kv_out, valid = projected[0], projected[1:-1], projected[-1]
    q_all = spread(q_own)
    kv_all = [kv_out[0]] + [swap(kv_out[r], "patch", r) for r in range(1, owners)]
    if share % 16:
        order = jnp.arange(owners) ^ me
        q_all = [jnp.take(jnp.stack(q_all), order, axis=0).reshape(WIDTH, span)]
        stacked = jnp.take(jnp.stack(kv_all), order, axis=0)
        kv_all = [stacked.transpose(1, 0, 2, 3).reshape(2, WIDTH, slots)]
    tile = min(512, span)
    count = len(q_all)
    q_full, acc, top, total = call(
        functools.partial(cached_kernel, count, tile),
        (
            shape(WIDTH, span),
            shape(WIDTH, span, dtype=jnp.float32),
            shape(8 * HEADS, span, dtype=jnp.float32),
            shape(8 * HEADS, span, dtype=jnp.float32),
        ),
        (ids, lengths[0], *q_all, cache_keys[0], cache_values[0]),
        smem=2,
        flops=4 * cache_keys.shape[1] * span * WIDTH,
        name="cached",
    )
    last = call(
        functools.partial(appended_kernel, count, owners, tile),
        (shape(slots, WIDTH), shape(slots, WIDTH)) + (shape(WIDTH + STAT_ROWS, rows),) * owners,
        (ids, *kv_all, valid, q_full, acc, top, total),
        smem=1,
        scratch=[
            pltpu.VMEM((WIDTH, slots), bf16),
            pltpu.VMEM((WIDTH, slots), bf16),
            pltpu.VMEM((WIDTH, span), bf16),
            pltpu.VMEM((STAT_ROWS, span), jnp.float32),
        ],
        flops=4 * slots * span * WIDTH,
        name="appended",
    )
    new_keys, new_values, parts = last[0], last[1], last[2:]
    far = sorted(range(1, owners), key=lambda r: (-bin(r >> 1).count("1"), r))
    got = {0: parts[0], **{r: swap(parts[r], "patch", r) for r in far}}
    attended = call(
        functools.partial(finish_kernel, owners),
        shape(rows, WIDTH),
        [got[r] for r in range(owners)],
        flops=4 * owners * rows * WIDTH,
        name="finish",
    )
    return attended[None], new_keys[None], new_values[None]


def solution(mesh):
    placed = (
        P("stream", "patch", None),
        P("stream", None),
        P("stream", None),
        P("stream", None),
        P("stream", "patch", None),
        P("stream", "patch", None),
        P("stream", "patch"),
        P("stream", "patch", None),
    )
    return jax.shard_map(
        body,
        mesh=mesh,
        in_specs=placed,
        out_specs=(
            P("stream", "patch", None),
            P("stream", "patch", None),
            P("stream", "patch", None),
        ),
        check_vma=False,
    )
```

```python
import functools
import math

import jax
import jax.numpy as jnp
from jax import lax
from jax.experimental import pallas as pl
from jax.experimental.pallas import tpu as pltpu
from jax.sharding import PartitionSpec as P


HEADS = 6
HD = 128
BLOCK = 128
APP = 4
EPS = 1e-06
MASKED = -1e30
WIDTH = HEADS * HD
EXP_SCALE = math.log2(math.e) / math.sqrt(HD)
STAT_ROWS = 32


VMEM = pl.BlockSpec(memory_space=pltpu.VMEM)
SMEM = pl.BlockSpec(memory_space=pltpu.SMEM)
ANY = pl.BlockSpec(memory_space=pl.ANY)
NT = (((1,), (1,)), ((), ()))
TN = (((0,), (0,)), ((), ()))


def call(kernel, out_shape, args, smem=0, hbm=0, scratch=(), sems=(), flops=0, limit=None):
    held = [*args[smem : len(args) - hbm], *jax.tree.leaves(out_shape), *scratch]
    size = sum(math.prod(x.shape) * jnp.dtype(x.dtype).itemsize for x in held)
    limit = limit or min(60 << 20, size * 5 // 4 + (10 << 20))
    return pl.pallas_call(
        kernel,
        out_shape=out_shape,
        in_specs=[SMEM] * smem + [VMEM] * (len(args) - smem - hbm) + [ANY] * hbm,
        out_specs=jax.tree.map(lambda _: VMEM, out_shape),
        scratch_shapes=[*scratch, *sems],
        compiler_params=pltpu.CompilerParams(vmem_limit_bytes=limit),
        cost_estimate=pl.CostEstimate(flops=flops, bytes_accessed=1 << 20, transcendentals=0),
    )(*args)


def place(device, owners):
    return jnp.bitwise_and(device, 1) * (owners // 2) + jnp.right_shift(device, 1)


def peer(axis, r):
    return jnp.bitwise_xor(lax.axis_index(axis).astype(jnp.int32), r)


def prepare_kernel(x_ref, wq_ref, wk_ref, wv_ref, x_out, wt_ref, w_scr, sems):
    share = wt_ref.shape[0] // 3
    window = w_scr.shape[2]
    first = peer("patch", 0) * share
    lanes = jnp.minimum(first - jnp.bitwise_and(first, 127), WIDTH - window)
    copies = []
    for i, w_ref in enumerate((wq_ref, wk_ref, wv_ref)):
        source = w_ref.at[:, pl.ds(pl.multiple_of(lanes, 128), window)]
        copies.append(pltpu.make_async_copy(source, w_scr.at[i], sems.at[i]))
        copies[-1].start()
    row = lax.broadcasted_iota(jnp.int32, (share, window), 0)
    col = lax.broadcasted_iota(jnp.int32, (share, window), 1)
    pick = (col == row + (first - lanes)).astype(jnp.float32).astype(jnp.bfloat16)
    floats = x_ref[...].astype(jnp.float32)
    mean = jnp.mean(floats * floats, axis=1, keepdims=True)
    x_out[...] = (floats * lax.rsqrt(mean + EPS)).astype(jnp.bfloat16)
    for i in range(3):
        copies[i].wait()
        part = lax.dot_general(pick, w_scr[i], NT, preferred_element_type=jnp.float32)
        wt_ref[i * share : (i + 1) * share, :] = part.astype(jnp.bfloat16)


def target_kernel(owners, most, assign_ref, tgt_ref):
    me = peer("patch", 0)
    groups = assign_ref.shape[1]
    owner = assign_ref[...]
    ids = lax.broadcasted_iota(jnp.int32, (max(owners, 8), groups), 0)
    named = (ids == owner).astype(jnp.float32)
    r = lax.broadcasted_iota(jnp.int32, (groups, groups), 0)
    c = lax.broadcasted_iota(jnp.int32, (groups, groups), 1)
    before = (r < c).astype(jnp.float32)
    seen = jnp.dot(named, before, preferred_element_type=jnp.float32)
    rank = jnp.sum(seen * named, axis=0, keepdims=True)
    token = lax.broadcasted_iota(jnp.int32, (groups, groups * APP), 1)
    group = lax.broadcasted_iota(jnp.int32, (groups, groups * APP), 0)
    mine = jnp.logical_and(token >= group * APP, token < group * APP + APP).astype(jnp.float32)
    both = jnp.concatenate(
        (
            jnp.broadcast_to(owner.astype(jnp.float32), (8, groups)),
            jnp.broadcast_to(rank, (8, groups)),
        ),
        axis=0,
    )
    both = jnp.dot(both, mine, preferred_element_type=jnp.float32).astype(jnp.int32)
    inner = jnp.bitwise_and(lax.broadcasted_iota(jnp.int32, tgt_ref.shape, 1), APP - 1)
    tgt_ref[...] = (both[0:8] * owners + me) * (most * APP) + both[8:16] * APP + inner


def project_kernel(owners, shards, *refs):
    x_refs, refs = refs[:owners], refs[owners:]
    w_refs, refs = refs[:shards], refs[shards:]
    q_ref, kv_ref, x_scr = refs
    rows = x_refs[0].shape[0]
    share = q_ref.shape[0]
    depth = w_refs[0].shape[1]
    for r in range(owners):
        at = pl.multiple_of(place(peer("patch", r), owners) * rows, rows)
        x_scr[pl.ds(at, rows), :] = x_refs[r][...]
    total = None
    for s in range(shards):
        at = pl.multiple_of(peer("stream", s) * depth, depth)
        part = lax.dot_general(
            w_refs[s][...], x_scr[:, pl.ds(at, depth)], NT, preferred_element_type=jnp.float32
        )
        total = part if total is None else total + part
    q_ref[...] = total[:share].astype(jnp.bfloat16)
    kv_ref[...] = total[share:].astype(jnp.bfloat16)


def select_kernel(owners, slots, *refs):
    t_refs, refs = refs[:owners], refs[owners:]
    kv_ref, refs = refs[0], refs[1:]
    kv_refs, (t_scr,) = refs[:owners], refs[owners:]
    rows = t_refs[0].shape[1]
    share = kv_ref.shape[0] // 2
    for r in range(owners):
        at = pl.multiple_of(place(peer("patch", r), owners) * rows, rows)
        t_scr[:, pl.ds(at, rows)] = t_refs[r][...]
    targets = t_scr[0:1, :]
    slot = lax.broadcasted_iota(jnp.int32, (slots, owners * rows), 0)
    for r in range(owners):
        hit = (slot == targets - peer("patch", r) * slots).astype(jnp.float32)
        got = lax.dot_general(
            kv_ref[...], hit.astype(jnp.bfloat16), NT, preferred_element_type=jnp.float32
        )
        kv_refs[r][0] = got[:share].astype(jnp.bfloat16)
        kv_refs[r][1] = got[share:].astype(jnp.bfloat16)


def occupied_kernel(slots, *refs):
    t_refs, valid_ref = refs[:-1], refs[-1]
    first = peer("patch", 0) * slots
    slot = lax.broadcasted_iota(jnp.int32, (slots, t_refs[0].shape[1]), 0)
    hits = [(slot == t_ref[0:1, :] - first).astype(jnp.float32) for t_ref in t_refs]
    hit = jnp.sum(functools.reduce(jnp.add, hits), axis=1, keepdims=True)
    valid_ref[...] = jnp.broadcast_to(hit, valid_ref.shape)


def each_tile(count, tile, one):
    if count <= 2:
        for j in range(count):
            one(j * tile)
    else:
        lax.fori_loop(
            0, count, lambda j, c: (one(pl.multiple_of(j * tile, tile)), c)[1], 0
        )


def cached_kernel(count, tile, len_ref, *refs):
    q_refs = refs[:count]
    k_ref, v_ref, q_all, acc_ref, top_ref, total_ref = refs[count:]
    if count == 1:
        q_all[...] = q_refs[0][...]
    else:
        share = q_refs[0].shape[0]
        for r in range(count):
            at = pl.multiple_of(peer("patch", r) * share, share)
            q_all[pl.ds(at, share), :] = q_refs[r][...]
    tokens = q_all.shape[1]
    length = len_ref[0]
    capacity = k_ref.shape[0]

    def run(keys, masked):
        def head(h, carry):
            at = pl.multiple_of(h * HD, HD)
            row = pl.multiple_of(h * 8, 8)
            key = k_ref[0:keys, pl.ds(at, HD)]
            value = v_ref[0:keys, pl.ds(at, HD)]

            def one(j):
                q = q_all[pl.ds(at, HD), pl.ds(j, tile)]
                s = jnp.dot(key, q, preferred_element_type=jnp.float32)
                if masked:
                    pos = lax.broadcasted_iota(jnp.int32, s.shape, 0)
                    s = jnp.where(pos < length * BLOCK, s, MASKED)
                top = jnp.max(s, axis=0, keepdims=True)
                w = jnp.exp2((s - top) * EXP_SCALE).astype(jnp.bfloat16)
                acc_ref[pl.ds(at, HD), pl.ds(j, tile)] = lax.dot_general(
                    value, w, TN, preferred_element_type=jnp.float32
                )
                total = jnp.sum(w.astype(jnp.float32), axis=0, keepdims=True)
                top_ref[pl.ds(row, 8), pl.ds(j, tile)] = jnp.broadcast_to(top, (8, tile))
                total_ref[pl.ds(row, 8), pl.ds(j, tile)] = jnp.broadcast_to(total, (8, tile))

            each_tile(tokens // tile, tile, one)
            return carry

        lax.fori_loop(0, HEADS, head, 0)

    short = min(2 * BLOCK, capacity)

    @pl.when(length * BLOCK <= short)
    def _():
        run(short, True)

    if capacity > short:

        @pl.when(jnp.logical_and(length * BLOCK > short, length * BLOCK < capacity))
        def _():
            run(capacity, True)

        @pl.when(jnp.logical_and(length * BLOCK > short, length * BLOCK >= capacity))
        def _():
            run(capacity, False)


def join_kernel(count, *refs):
    kv_refs, (nk_ref, nv_ref, vt_ref, kt_scr) = refs[:count], refs[count:]
    if count == 1:
        kt_scr[...] = kv_refs[0][0]
        vt_ref[...] = kv_refs[0][1]
    else:
        share = kv_refs[0].shape[1]
        for r in range(count):
            at = pl.multiple_of(peer("patch", r) * share, share)
            kt_scr[pl.ds(at, share), :] = kv_refs[r][0]
            vt_ref[pl.ds(at, share), :] = kv_refs[r][1]
    nk_ref[...] = kt_scr[...].astype(jnp.float32).T.astype(jnp.bfloat16)
    nv_ref[...] = vt_ref[...].astype(jnp.float32).T.astype(jnp.bfloat16)


def levels_to_rows(level, stat_ref, h, j, tile):
    high = level.astype(jnp.bfloat16).astype(jnp.float32)
    middle = (level - high).astype(jnp.bfloat16).astype(jnp.float32)
    stat_ref[h : h + 1, pl.ds(j, tile)] = high
    stat_ref[8 + h : 9 + h, pl.ds(j, tile)] = middle
    stat_ref[16 + h : 17 + h, pl.ds(j, tile)] = level - high - middle


def rows_to_levels(stat):
    stat = stat.astype(jnp.float32)
    return stat[0:8] + stat[8:16] + stat[16:24]


def appended_kernel(other, tile, nk_ref, vt_ref, valid_ref, q_ref, acc_ref, top_ref, total_ref,
                    out_ref, stat_scr):
    half = out_ref.shape[1]
    core = jnp.bitwise_and(peer("patch", other), 1)
    bias = jnp.where(valid_ref[:, 0:1] > 0.5, 0.0, MASKED)
    stat_scr[...] = jnp.zeros_like(stat_scr)

    def one(h, j):
        lo, hi = h * HD, (h + 1) * HD
        at = pl.multiple_of(core * half + j, tile)
        q = q_ref[lo:hi, pl.ds(at, tile)]
        s = jnp.dot(nk_ref[:, lo:hi], q, preferred_element_type=jnp.float32) + bias
        old_top = top_ref[8 * h : 8 * h + 1, pl.ds(at, tile)]
        top = jnp.maximum(jnp.max(s, axis=0, keepdims=True), old_top)
        w = jnp.exp2((s - top) * EXP_SCALE).astype(jnp.bfloat16)
        numer = jnp.dot(vt_ref[lo:hi, :], w, preferred_element_type=jnp.float32)
        old = jnp.exp2((old_top - top) * EXP_SCALE)
        total = (
            jnp.sum(w.astype(jnp.float32), axis=0, keepdims=True)
            + total_ref[8 * h : 8 * h + 1, pl.ds(at, tile)] * old
        )
        inverse = 1.0 / total
        mixed = acc_ref[lo:hi, pl.ds(at, tile)] * (old * inverse) + numer * inverse
        out_ref[lo:hi, pl.ds(j, tile)] = mixed.astype(jnp.bfloat16)
        levels_to_rows(top * EXP_SCALE + jnp.log2(total), stat_scr, h, j, tile)

    for h in range(HEADS):
        each_tile(half // tile, tile, functools.partial(one, h))
    out_ref[WIDTH:, :] = stat_scr[...].astype(jnp.bfloat16)


def combine_kernel(owners, a_ref, b_ref, *refs):
    out_refs, (out_scr, stat_scr) = refs[: owners // 2], refs[owners // 2 :]
    half = a_ref.shape[1]
    la, lb = rows_to_levels(a_ref[WIDTH:, :]), rows_to_levels(b_ref[WIDTH:, :])
    best = jnp.maximum(la, lb)
    fa, fb = jnp.exp2(la - best), jnp.exp2(lb - best)
    total = fa + fb
    inverse = 1.0 / total
    fa, fb = fa * inverse, fb * inverse
    level = best + jnp.log2(total)
    stat_scr[...] = jnp.zeros_like(stat_scr)
    for h in range(HEADS):
        lo, hi = h * HD, (h + 1) * HD
        mixed = (
            a_ref[lo:hi, :].astype(jnp.float32) * fa[h : h + 1, :]
            + b_ref[lo:hi, :].astype(jnp.float32) * fb[h : h + 1, :]
        )
        out_scr[lo:hi, :] = mixed.astype(jnp.bfloat16)
        levels_to_rows(level[h : h + 1, :], stat_scr, h, 0, half)
    out_scr[WIDTH:, :] = stat_scr[...].astype(jnp.bfloat16)
    rows = half // (owners // 2)
    for r in range(owners // 2):
        at = pl.multiple_of(jnp.right_shift(peer("patch", 2 * r), 1) * rows, rows)
        out_refs[r][...] = out_scr[:, pl.ds(at, rows)]


def finish_kernel(count, *refs):
    got, out_ref = refs[:count], refs[count]
    levels = [rows_to_levels(got[r][WIDTH:, :]) for r in range(count)]
    best = functools.reduce(jnp.maximum, levels)
    factors = [jnp.exp2(level - best) for level in levels]
    inverse = 1.0 / functools.reduce(jnp.add, factors)
    factors = [factor * inverse for factor in factors]
    for h in range(HEADS):
        lo, hi = h * HD, (h + 1) * HD
        mixed = None
        for r in range(count):
            part = got[r][lo:hi, :].astype(jnp.float32) * factors[r][h : h + 1, :]
            mixed = part if mixed is None else mixed + part
        out_ref[:, lo:hi] = mixed.T.astype(jnp.bfloat16)


def body(tokens, query_weight, key_weight, value_weight, cache_keys, cache_values, lengths, assign):
    owners = lax.axis_size("patch")
    shards = lax.axis_size("stream")
    rows = tokens.shape[1]
    groups = rows // APP
    most = max(2, 2 * groups // owners)
    slots = owners * most * APP
    share = WIDTH // owners
    span = owners * rows
    half = span // 2
    chips = owners // 2
    depth = query_weight.shape[0]
    bf16, f32 = jnp.bfloat16, jnp.float32

    def shape(*dims, dtype=bf16):
        return jax.ShapeDtypeStruct(dims, dtype)

    def swap(x, axis, r):
        size = lax.axis_size(axis)
        return lax.ppermute(x, axis, [(i, i ^ r) for i in range(size)])

    def far_first(ids):
        return sorted(ids, key=lambda r: (-bin(r >> 1).count("1"), r))

    def spread(x):
        got = {0: x}
        for r in far_first(range(2, owners, 2)):
            got[r] = swap(x, "patch", r)
        for r in range(0, owners, 2):
            got[r + 1] = swap(got[r], "patch", 1)
        return [got[r] for r in range(owners)]

    normed, wt = call(
        prepare_kernel,
        (shape(rows, tokens.shape[2]), shape(3 * share, depth)),
        (tokens[0], query_weight, key_weight, value_weight),
        hbm=3,
        scratch=[pltpu.VMEM((3, depth, min(WIDTH, 256)), bf16)],
        sems=[pltpu.SemaphoreType.DMA((3,))],
        flops=6 * share * WIDTH * depth,
        limit=60 << 20,
    )
    w_all = [wt] + [swap(wt, "stream", s) for s in range(1, shards)]
    tgt = call(
        functools.partial(target_kernel, owners, most),
        shape(8, rows, dtype=jnp.int32),
        (assign.reshape(1, groups),),
        flops=1 << 20,
    )
    x_all = spread(normed)
    t_all = spread(tgt)
    q_own, kv_own = call(
        functools.partial(project_kernel, owners, shards),
        (shape(share, span), shape(2 * share, span)),
        (*x_all, *w_all),
        scratch=[pltpu.VMEM((span, shards * depth), bf16)],
        flops=6 * share * span * shards * depth,
    )
    q_all = spread(q_own)
    kv_out = call(
        functools.partial(select_kernel, owners, slots),
        (shape(2, share, slots),) * owners,
        (*t_all, kv_own),
        scratch=[pltpu.VMEM((8, span), jnp.int32)],
        flops=4 * share * span * slots * owners,
    )
    valid = call(
        functools.partial(occupied_kernel, slots),
        shape(slots, 128, dtype=f32),
        t_all,
        flops=1 << 20,
    )
    kv_all = {0: kv_out[0]}
    for r in far_first(range(1, owners)):
        kv_all[r] = swap(kv_out[r], "patch", r)
    kv_all = [kv_all[r] for r in range(owners)]
    if share % 16:
        order = jnp.arange(owners) ^ lax.axis_index("patch")
        q_all = [jnp.take(jnp.stack(q_all), order, axis=0).reshape(WIDTH, span)]
        stacked = jnp.take(jnp.stack(kv_all), order, axis=0)
        kv_all = [stacked.transpose(1, 0, 2, 3).reshape(2, WIDTH, slots)]
    tile = min(512, half)
    count = len(q_all)
    q_full, acc, top, total = call(
        functools.partial(cached_kernel, count, tile),
        (
            shape(WIDTH, span),
            shape(WIDTH, span, dtype=f32),
            shape(8 * HEADS, span, dtype=f32),
            shape(8 * HEADS, span, dtype=f32),
        ),
        (lengths[0], *q_all, cache_keys[0], cache_values[0]),
        smem=1,
        flops=4 * cache_keys.shape[1] * span * WIDTH,
    )
    new_keys, new_values, vt = call(
        functools.partial(join_kernel, count),
        (shape(slots, WIDTH), shape(slots, WIDTH), shape(WIDTH, slots)),
        kv_all,
        scratch=[pltpu.VMEM((WIDTH, slots), bf16)],
        flops=1 << 20,
    )

    def appended(other):
        return call(
            functools.partial(appended_kernel, other, tile),
            shape(WIDTH + STAT_ROWS, half),
            (new_keys, vt, valid, q_full, acc, top, total),
            scratch=[pltpu.VMEM((STAT_ROWS, half), f32)],
            flops=4 * slots * half * WIDTH,
        )

    theirs = swap(appended(1), "patch", 1)
    parts = call(
        functools.partial(combine_kernel, owners),
        (shape(WIDTH + STAT_ROWS, rows),) * chips,
        (appended(0), theirs),
        scratch=[
            pltpu.VMEM((WIDTH + STAT_ROWS, half), bf16),
            pltpu.VMEM((STAT_ROWS, half), f32),
        ],
        flops=4 * half * WIDTH,
    )
    got = [parts[0]] + [None] * (chips - 1)
    for r in far_first(range(2, owners, 2)):
        got[r // 2] = swap(parts[r // 2], "patch", r)
    attended = call(
        functools.partial(finish_kernel, chips),
        shape(rows, WIDTH),
        got,
        flops=4 * chips * rows * WIDTH,
    )
    return attended[None], new_keys[None], new_values[None]


def solution(mesh):
    placed = (
        P("stream", "patch", None),
        P("stream", None),
        P("stream", None),
        P("stream", None),
        P("stream", "patch", None),
        P("stream", "patch", None),
        P("stream", "patch"),
        P("stream", "patch", None),
    )
    return jax.shard_map(
        body,
        mesh=mesh,
        in_specs=placed,
        out_specs=(
            P("stream", "patch", None),
            P("stream", "patch", None),
            P("stream", "patch", None),
        ),
        check_vma=False,
    )
```

```python
import functools
import math

import jax
import jax.numpy as jnp
from jax import lax
from jax.experimental import pallas as pl
from jax.experimental.pallas import tpu as pltpu
from jax.sharding import PartitionSpec as P


HEADS = 6
HD = 128
BLOCK = 128
APP = 4
EPS = 1e-06
MASKED = -1e30
WIDTH = HEADS * HD
EXP_SCALE = math.log2(math.e) / math.sqrt(HD)
STAT_ROWS = 32


VMEM = pl.BlockSpec(memory_space=pltpu.VMEM)
SMEM = pl.BlockSpec(memory_space=pltpu.SMEM)
ANY = pl.BlockSpec(memory_space=pl.ANY)
NT = (((1,), (1,)), ((), ()))
TN = (((0,), (0,)), ((), ()))


def call(kernel, out_shape, args, smem=0, hbm=0, scratch=(), sems=(), flops=0, limit=None):
    held = [*args[smem : len(args) - hbm], *jax.tree.leaves(out_shape), *scratch]
    size = sum(math.prod(x.shape) * jnp.dtype(x.dtype).itemsize for x in held)
    limit = limit or min(60 << 20, size * 5 // 4 + (10 << 20))
    return pl.pallas_call(
        kernel,
        out_shape=out_shape,
        in_specs=[SMEM] * smem + [VMEM] * (len(args) - smem - hbm) + [ANY] * hbm,
        out_specs=jax.tree.map(lambda _: VMEM, out_shape),
        scratch_shapes=[*scratch, *sems],
        compiler_params=pltpu.CompilerParams(vmem_limit_bytes=limit),
        cost_estimate=pl.CostEstimate(flops=flops, bytes_accessed=1 << 20, transcendentals=0),
    )(*args)


def peer(axis, r):
    return jnp.bitwise_xor(lax.axis_index(axis).astype(jnp.int32), r)


def chip(s):
    return jnp.right_shift(peer("patch", 2 * s), 1)


def core(j):
    return jnp.bitwise_and(peer("patch", j), 1)


def part(index, size):
    return pl.ds(pl.multiple_of(index * size, size), size)


def normalize_kernel(x_ref, x_out):
    floats = x_ref[...].astype(jnp.float32)
    mean = jnp.mean(floats * floats, axis=1, keepdims=True)
    x_out[...] = (floats * lax.rsqrt(mean + EPS)).astype(jnp.bfloat16)


def columns_kernel(wq_ref, wk_ref, wv_ref, wq_out, wkv_out, w_scr, sems):
    share = wq_out.shape[0]
    window = w_scr.shape[2]
    first = peer("patch", 0) * share
    lanes = jnp.minimum(first - jnp.bitwise_and(first, 127), WIDTH - window)
    copies = []
    for i, w_ref in enumerate((wq_ref, wk_ref, wv_ref)):
        source = w_ref.at[:, pl.ds(pl.multiple_of(lanes, 128), window)]
        copies.append(pltpu.make_async_copy(source, w_scr.at[i], sems.at[i]))
        copies[-1].start()
    row = lax.broadcasted_iota(jnp.int32, (share, window), 0)
    col = lax.broadcasted_iota(jnp.int32, (share, window), 1)
    pick = (col == row + (first - lanes)).astype(jnp.float32).astype(jnp.bfloat16)
    got = []
    for i in range(3):
        copies[i].wait()
        got.append(lax.dot_general(pick, w_scr[i], NT, preferred_element_type=jnp.float32))
    wq_out[...] = got[0].astype(jnp.bfloat16)
    wkv_out[...] = jnp.concatenate(got[1:], axis=0).astype(jnp.bfloat16)


def target_kernel(owners, most, assign_ref, tgt_ref):
    groups = assign_ref.shape[1]
    owner = assign_ref[...]
    ids = lax.broadcasted_iota(jnp.int32, (max(owners, 8), groups), 0)
    named = (ids == owner).astype(jnp.float32)
    r = lax.broadcasted_iota(jnp.int32, (groups, groups), 0)
    c = lax.broadcasted_iota(jnp.int32, (groups, groups), 1)
    before = (r < c).astype(jnp.float32)
    seen = jnp.dot(named, before, preferred_element_type=jnp.float32)
    rank = jnp.sum(seen * named, axis=0, keepdims=True)
    token = lax.broadcasted_iota(jnp.int32, (groups, groups * APP), 1)
    group = lax.broadcasted_iota(jnp.int32, (groups, groups * APP), 0)
    mine = jnp.logical_and(token >= group * APP, token < group * APP + APP).astype(jnp.float32)
    both = jnp.concatenate(
        (
            jnp.broadcast_to(owner.astype(jnp.float32), (8, groups)),
            jnp.broadcast_to(rank, (8, groups)),
        ),
        axis=0,
    )
    both = jnp.dot(both, mine, preferred_element_type=jnp.float32).astype(jnp.int32)
    inner = jnp.bitwise_and(lax.broadcasted_iota(jnp.int32, tgt_ref.shape, 1), APP - 1)
    source = both[0:8] * (owners // 2) + chip(0)
    tgt_ref[...] = source * (most * APP) + both[8:16] * APP + inner


def stage_kernel(k0_ref, v0_ref, k1_ref, v1_ref, kk_ref, vt_ref, v_scr, sems):
    copies = [
        pltpu.make_async_copy(v0_ref, v_scr.at[0], sems.at[0]),
        pltpu.make_async_copy(v1_ref, v_scr.at[1], sems.at[1]),
        pltpu.make_async_copy(k0_ref, kk_ref.at[0], sems.at[2]),
        pltpu.make_async_copy(k1_ref, kk_ref.at[1], sems.at[3]),
    ]
    for copy in copies:
        copy.start()
    for j in range(2):
        copies[j].wait()
        for h in range(HEADS):
            lo, hi = h * HD, (h + 1) * HD
            vt_ref[j, lo:hi, :] = v_scr[j, :, lo:hi].astype(jnp.float32).T.astype(jnp.bfloat16)
    copies[2].wait()
    copies[3].wait()


def gather_weights_kernel(shards, kinds, *refs):
    w_refs, (out_ref, scr) = refs[: 2 * shards], refs[2 * shards :]
    share, depth = w_refs[0].shape[0] // kinds, w_refs[0].shape[1]
    for j in range(2):
        for s in range(shards):
            for i in range(kinds):
                rows = part(core(j) + 2 * i, share)
                piece = w_refs[j * shards + s][...].astype(jnp.float32)
                scr[rows, part(peer("stream", s), depth)] = piece[i * share : (i + 1) * share]
    out_ref[...] = scr[...].astype(jnp.bfloat16)


def project_q_kernel(chips, *refs):
    x_refs, (w_ref, q_ref, x_ref) = refs[:chips], refs[chips:]
    rows = x_refs[0].shape[0]
    for s in range(chips):
        x_ref[part(chip(s), rows), :] = x_refs[s][...]
    q_ref[...] = lax.dot_general(
        w_ref[...], x_ref[...], NT, preferred_element_type=jnp.float32
    ).astype(jnp.bfloat16)


def project_kv_kernel(chips, x_ref, w_ref, kv_ref, *out_refs):
    kv_ref[...] = lax.dot_general(
        w_ref[...], x_ref[...], NT, preferred_element_type=jnp.float32
    ).astype(jnp.bfloat16)
    wide = kv_ref.shape[0] // 2
    rows = x_ref.shape[0] // chips
    for s in range(chips):
        out_refs[s][0] = kv_ref[0:wide, part(chip(s), rows)]
        out_refs[s][1] = kv_ref[wide:, part(chip(s), rows)]


def hits_kernel(chips, *refs):
    t_refs, refs = refs[:chips], refs[chips:]
    out_refs, (t_scr,) = refs[:chips], refs[chips:]
    rows = t_refs[0].shape[1]
    for s in range(chips):
        t_scr[:, part(chip(s), rows)] = t_refs[s][...]
    targets = t_scr[0:1, :]
    slots = out_refs[0].shape[0]
    slot = lax.broadcasted_iota(jnp.int32, (slots, chips * rows), 0)
    for s in range(chips):
        hit = slot == targets - chip(s) * slots
        out_refs[s][...] = hit.astype(jnp.float32).astype(jnp.bfloat16)


def select_kernel(chips, *refs):
    hit_refs, (kv_ref, *out_refs) = refs[:chips], refs[chips:]
    wide = kv_ref.shape[0] // 2
    for s in range(chips):
        got = lax.dot_general(
            kv_ref[...], hit_refs[s][...], NT, preferred_element_type=jnp.float32
        )
        out_refs[s][0] = got[:wide].astype(jnp.bfloat16)
        out_refs[s][1] = got[wide:].astype(jnp.bfloat16)


def each_tile(count, tile, one):
    if count <= 2:
        for j in range(count):
            one(j * tile)
    else:
        lax.fori_loop(
            0, count, lambda j, c: (one(pl.multiple_of(j * tile, tile)), c)[1], 0
        )


def head_group(chips, flip):
    top = jnp.bitwise_and(chip(0), chips // 2) > 0
    return jnp.where(top, 1 - flip, flip) * (HEADS // 2)


def with_ones(value):
    return jnp.concatenate((value, jnp.ones((16, value.shape[1]), value.dtype)), axis=0)


def cached_kernel(chips, flip, tile, len0_ref, len1_ref, *refs):
    q_refs, refs = refs[: chips // 2], refs[chips // 2 :]
    kk_ref, vt_ref, q_all, acc_ref, top_ref, total_ref = refs
    wide = q_refs[0].shape[0]
    for i in range(chips // 2):
        at = jnp.bitwise_and(chip(i), chips // 2 - 1)
        q_all[part(at, wide), :] = q_refs[i][...]
    tokens = q_all.shape[1]
    capacity = kk_ref.shape[1]
    short = min(2 * BLOCK, capacity)
    first = head_group(chips, flip)
    lengths = (len0_ref[0], len1_ref[0])

    def run(sizes):
        def head(h, carry):
            at = part(h, HD)
            row = part(h, 8)
            keys = [kk_ref[i, 0 : sizes[i], part(first + h, HD)] for i in range(2)]
            values = [with_ones(vt_ref[i, part(first + h, HD), 0 : sizes[i]]) for i in range(2)]

            def several(j):
                lanes = [pl.ds(j + t * tile, tile) for t in range(min(2, tokens // tile))]
                scores = []
                for lane in lanes:
                    q = q_all[at, lane]
                    both = []
                    for i in range(2):
                        s = jnp.dot(keys[i], q, preferred_element_type=jnp.float32)
                        if sizes[i] == short:
                            pos = lax.broadcasted_iota(jnp.int32, s.shape, 0)
                            s = jnp.where(pos < lengths[i] * BLOCK, s, MASKED)
                        both.append(s)
                    scores.append(both)
                tops = [
                    jnp.maximum(*[jnp.max(s, axis=0, keepdims=True) for s in both])
                    for both in scores
                ]
                weights = [
                    [jnp.exp2((s - top) * EXP_SCALE).astype(jnp.bfloat16) for s in both]
                    for both, top in zip(scores, tops)
                ]
                numers = [
                    sum(
                        jnp.dot(v, w, preferred_element_type=jnp.float32)
                        for v, w in zip(values, both)
                    )
                    for both in weights
                ]
                for lane, top, numer in zip(lanes, tops, numers):
                    acc_ref[at, lane] = numer[:HD]
                    top_ref[row, lane] = jnp.broadcast_to(top, (8, tile))
                    total_ref[row, lane] = numer[HD : HD + 8]

            step = min(2 * tile, tokens)
            each_tile(tokens // step, step, several)
            return carry

        lax.fori_loop(0, HEADS // 2, head, 0)

    brief = [length * BLOCK <= short for length in lengths]
    if capacity <= short:
        run((short, short))
    else:
        for sizes in ((short, short), (short, capacity), (capacity, short), (capacity, capacity)):
            want = [size == short for size in sizes]
            fits = [b if w else jnp.logical_not(b) for b, w in zip(brief, want)]

            @pl.when(jnp.logical_and(*fits))
            def _(sizes=sizes):
                run(sizes)


def rows_to_levels(stat):
    stat = stat.astype(jnp.float32)
    return stat[0:8] + stat[8:16] + stat[16:24]


def appended_kernel(chips, tile, *refs):
    kv_refs, refs = refs[: 2 * chips], refs[2 * chips :]
    states, refs = (refs[0:4], refs[4:8]), refs[8:]
    out_refs, (kt_scr, vt_scr, out_scr, level_scr) = refs[:chips], refs[chips:]
    wide, rows = kv_refs[0].shape[1], kv_refs[0].shape[2]
    for j in range(2):
        for s in range(chips):
            kt_scr[part(chip(s), wide), j * rows : (j + 1) * rows] = kv_refs[j * chips + s][0]
            vt_scr[part(chip(s), wide), j * rows : (j + 1) * rows] = kv_refs[j * chips + s][1]
    tokens = level_scr.shape[1]

    def several(j):
        lanes = pl.ds(j, tile)
        units = [(flip, h) for flip in range(2) for h in range(HEADS // 2)]
        heads = [head_group(chips, flip) + h for flip, h in units]
        scores = [
            lax.dot_general(
                kt_scr[part(head, HD), :],
                states[flip][0][h * HD : (h + 1) * HD, lanes],
                TN,
                preferred_element_type=jnp.float32,
            )
            for (flip, h), head in zip(units, heads)
        ]
        olds = [states[flip][2][8 * h : 8 * h + 1, lanes] for flip, h in units]
        tops = [jnp.maximum(jnp.max(s, axis=0, keepdims=True), o) for s, o in zip(scores, olds)]
        weights = [
            jnp.exp2((s - top) * EXP_SCALE).astype(jnp.bfloat16) for s, top in zip(scores, tops)
        ]
        numers = [
            jnp.dot(with_ones(vt_scr[part(head, HD), :]), w, preferred_element_type=jnp.float32)
            for head, w in zip(heads, weights)
        ]
        row = lax.broadcasted_iota(jnp.int32, (8, tile), 0)
        levels = jnp.zeros((8, tile), jnp.float32)
        for (flip, h), head, old_top, top, numer in zip(units, heads, olds, tops, numers):
            old = jnp.exp2((old_top - top) * EXP_SCALE)
            total = numer[HD : HD + 1] + states[flip][3][8 * h : 8 * h + 1, lanes] * old
            inverse = 1.0 / total
            mixed = states[flip][1][h * HD : (h + 1) * HD, lanes] * (old * inverse)
            mixed = mixed + numer[:HD] * inverse
            out_scr[part(head, HD), lanes] = mixed.astype(jnp.bfloat16)
            levels = jnp.where(row == head, top * EXP_SCALE + jnp.log2(total), levels)
        level_scr[:, lanes] = levels

    each_tile(tokens // tile, tile, several)
    level = level_scr[...]
    high = level.astype(jnp.bfloat16)
    rest = level - high.astype(jnp.float32)
    middle = rest.astype(jnp.bfloat16)
    low = rest - middle.astype(jnp.float32)
    stat = jnp.concatenate(
        (high.astype(jnp.float32), middle.astype(jnp.float32), low, jnp.zeros_like(low)), axis=0
    )
    out_scr[WIDTH:, :] = stat.astype(jnp.bfloat16)
    count = tokens // chips
    for s in range(chips):
        out_refs[s][...] = out_scr[:, part(chip(s), count)]


def regroup_kernel(chips, *refs):
    kv_refs, (mine_ref, other_ref) = refs[:chips], refs[chips:]
    wide, slots = kv_refs[0].shape[1], kv_refs[0].shape[2] // 2
    for s in range(chips):
        for i in range(2):
            mine_ref[i, part(chip(s), wide), :] = kv_refs[s][i, :, part(core(0), slots)]
            other_ref[i, part(chip(s), wide), :] = kv_refs[s][i, :, part(core(1), slots)]


def join_kernel(chips, mine_ref, got_ref, nk_ref, nv_ref, scr):
    size = mine_ref.shape[2] // chips
    for i, out_ref in enumerate((nk_ref, nv_ref)):
        for j, ref in enumerate((mine_ref, got_ref)):
            rows = ref[i].astype(jnp.float32).T
            for c in range(chips):
                scr[part(core(j) + 2 * c, size), :] = rows[c * size : (c + 1) * size]
        out_ref[...] = scr[...].astype(jnp.bfloat16)


def finish_kernel(count, *refs):
    got, out_ref = refs[:count], refs[count]
    levels = [rows_to_levels(got[r][WIDTH:, :]) for r in range(count)]
    best = functools.reduce(jnp.maximum, levels)
    factors = [jnp.exp2(level - best) for level in levels]
    inverse = 1.0 / functools.reduce(jnp.add, factors)
    factors = [factor * inverse for factor in factors]
    for h in range(HEADS):
        lo, hi = h * HD, (h + 1) * HD
        mixed = None
        for r in range(count):
            piece = got[r][lo:hi, :].astype(jnp.float32) * factors[r][h : h + 1, :]
            mixed = piece if mixed is None else mixed + piece
        out_ref[:, lo:hi] = mixed.T.astype(jnp.bfloat16)


def body(tokens, query_weight, key_weight, value_weight, cache_keys, cache_values, lengths, assign):
    owners = lax.axis_size("patch")
    shards = lax.axis_size("stream")
    chips = owners // 2
    rows, features = tokens.shape[1:]
    groups = rows // APP
    most = max(2, 2 * groups // owners)
    slots = chips * most * APP
    share = WIDTH // owners
    wide = WIDTH // chips
    half = chips * rows
    depth = query_weight.shape[0]
    cached_rows = cache_keys.shape[1]
    bf16, f32 = jnp.bfloat16, jnp.float32

    def shape(*dims, dtype=bf16):
        return jax.ShapeDtypeStruct(dims, dtype)

    def swap(x, axis, r):
        size = lax.axis_size(axis)
        return lax.ppermute(x, axis, [(i, i ^ r) for i in range(size)])

    def twin(x):
        return swap(x, "patch", 1)

    def far(parts, order=None):
        got = {0: parts[0]}
        for s in order or range(chips - 1, 0, -1):
            got[s] = swap(parts[s], "patch", 2 * s)
        return [got[s] for s in range(chips)]

    normed = call(normalize_kernel, shape(rows, features), (tokens[0],), flops=4 * rows * features)
    x_all = far([normed] * chips)
    wq, wkv = call(
        columns_kernel,
        (shape(share, depth), shape(2 * share, depth)),
        (query_weight, key_weight, value_weight),
        hbm=3,
        scratch=[pltpu.VMEM((3, depth, min(WIDTH, 256)), bf16)],
        sems=[pltpu.SemaphoreType.DMA((3,))],
        flops=6 * share * WIDTH * depth,
        limit=60 << 20,
    )
    wq_all = [wq] + [swap(wq, "stream", s) for s in range(1, shards)]
    wkv_all = [wkv] + [swap(wkv, "stream", s) for s in range(1, shards)]
    other_keys = twin(cache_keys[0])
    other_values = twin(cache_values[0])
    other_length = twin(lengths)
    tgt = call(
        functools.partial(target_kernel, owners, most),
        shape(8, rows, dtype=jnp.int32),
        (assign.reshape(1, groups),),
        flops=1 << 20,
    )
    t_all = far([tgt] * chips)
    kk, vt = call(
        stage_kernel,
        (shape(2, cached_rows, WIDTH), shape(2, WIDTH, cached_rows)),
        (cache_keys[0], cache_values[0], other_keys, other_values),
        hbm=4,
        scratch=[pltpu.VMEM((2, cached_rows, WIDTH), bf16)],
        sems=[pltpu.SemaphoreType.DMA((4,))],
        flops=1 << 20,
    )

    def whole(parts, kinds):
        parts = parts + [twin(p) for p in parts]
        return call(
            functools.partial(gather_weights_kernel, shards, kinds),
            shape(kinds * wide, shards * depth),
            parts,
            scratch=[pltpu.VMEM((kinds * wide, shards * depth), f32)],
            flops=1 << 20,
        )

    wq_full = whole(wq_all, 1)
    q_own, x_full = call(
        functools.partial(project_q_kernel, chips),
        (shape(wide, half), shape(half, features)),
        (*x_all, wq_full),
        flops=2 * wide * half * features,
    )
    near = list(range(1, chips // 2)) + list(range(chips // 2, chips))
    q_all = far([q_own] * chips, order=near)
    wkv_full = whole(wkv_all, 2)
    projected = call(
        functools.partial(project_kv_kernel, chips),
        (shape(2 * wide, half),) + (shape(2, wide, rows),) * chips,
        (x_full, wkv_full),
        flops=4 * wide * half * features,
    )
    kv_own, dense = projected[0], far(projected[1:])
    dense = dense + [twin(d) for d in dense]
    hits = call(
        functools.partial(hits_kernel, chips),
        (shape(2 * slots, half),) * chips,
        t_all,
        scratch=[pltpu.VMEM((8, half), jnp.int32)],
        flops=1 << 20,
    )
    selected = call(
        functools.partial(select_kernel, chips),
        (shape(2, wide, 2 * slots),) * chips,
        (*hits, kv_own),
        flops=8 * wide * half * slots * chips,
    )
    sent = far(selected)
    tile = min(256, half)

    def cached(flip):
        first = flip * (chips // 2)
        return call(
            functools.partial(cached_kernel, chips, flip, tile),
            (
                shape(WIDTH // 2, half),
                shape(WIDTH // 2, half, dtype=f32),
                shape(4 * HEADS, half, dtype=f32),
                shape(4 * HEADS, half, dtype=f32),
            ),
            (lengths[0], other_length[0], *q_all[first : first + chips // 2], kk, vt),
            smem=2,
            flops=4 * cached_rows * half * WIDTH,
        )

    states = [*cached(0), *cached(1)]
    parts = call(
        functools.partial(appended_kernel, chips, min(512, half)),
        (shape(WIDTH + STAT_ROWS, rows),) * chips,
        (*dense, *states),
        scratch=[
            pltpu.VMEM((WIDTH, 2 * rows), bf16),
            pltpu.VMEM((WIDTH, 2 * rows), bf16),
            pltpu.VMEM((WIDTH + STAT_ROWS, half), bf16),
            pltpu.VMEM((8, half), f32),
        ],
        flops=8 * rows * half * WIDTH,
    )
    got = far(parts)
    mine, other = call(
        functools.partial(regroup_kernel, chips), (shape(2, WIDTH, slots),) * 2, sent, flops=1 << 20
    )
    new_keys, new_values = call(
        functools.partial(join_kernel, chips),
        (shape(2 * slots, WIDTH),) * 2,
        (mine, twin(other)),
        scratch=[pltpu.VMEM((2 * slots, WIDTH), f32)],
        flops=1 << 20,
    )
    attended = call(
        functools.partial(finish_kernel, chips),
        shape(rows, WIDTH),
        got,
        flops=4 * chips * rows * WIDTH,
    )
    return attended[None], new_keys[None], new_values[None]


def solution(mesh):
    placed = (
        P("stream", "patch", None),
        P("stream", None),
        P("stream", None),
        P("stream", None),
        P("stream", "patch", None),
        P("stream", "patch", None),
        P("stream", "patch"),
        P("stream", "patch", None),
    )
    return jax.shard_map(
        body,
        mesh=mesh,
        in_specs=placed,
        out_specs=(
            P("stream", "patch", None),
            P("stream", "patch", None),
            P("stream", "patch", None),
        ),
        check_vma=False,
    )
```

```python
import functools
import math

import jax
import jax.numpy as jnp
from jax import lax
from jax.experimental import pallas as pl
from jax.experimental.pallas import tpu as pltpu
from jax.sharding import PartitionSpec as P


HEADS = 6
HD = 128
BLOCK = 128
APP = 4
EPS = 1e-06
MASKED = -1e30
WIDTH = HEADS * HD
EXP_SCALE = math.log2(math.e) / math.sqrt(HD)
STAT_ROWS = 32


VMEM = pl.BlockSpec(memory_space=pltpu.VMEM)
SMEM = pl.BlockSpec(memory_space=pltpu.SMEM)
ANY = pl.BlockSpec(memory_space=pl.ANY)
NT = (((1,), (1,)), ((), ()))
TN = (((0,), (0,)), ((), ()))


def call(kernel, out_shape, args, smem=0, hbm=0, scratch=(), sems=(), flops=0, limit=None):
    held = [*args[smem : len(args) - hbm], *jax.tree.leaves(out_shape), *scratch]
    size = sum(math.prod(x.shape) * jnp.dtype(x.dtype).itemsize for x in held)
    limit = limit or min(60 << 20, size * 5 // 4 + (10 << 20))
    return pl.pallas_call(
        kernel,
        out_shape=out_shape,
        in_specs=[SMEM] * smem + [VMEM] * (len(args) - smem - hbm) + [ANY] * hbm,
        out_specs=jax.tree.map(lambda _: VMEM, out_shape),
        scratch_shapes=[*scratch, *sems],
        compiler_params=pltpu.CompilerParams(vmem_limit_bytes=limit),
        cost_estimate=pl.CostEstimate(flops=flops, bytes_accessed=1 << 20, transcendentals=0),
    )(*args)


def peer(axis, r):
    return jnp.bitwise_xor(lax.axis_index(axis).astype(jnp.int32), r)


def chip(s):
    return jnp.right_shift(peer("patch", 2 * s), 1)


def core(j):
    return jnp.bitwise_and(peer("patch", j), 1)


def part(index, size):
    if isinstance(index, int):
        return slice(index * size, (index + 1) * size)
    return pl.ds(pl.multiple_of(index * size, size), size)


def normalize_kernel(x_ref, x_out):
    floats = x_ref[...].astype(jnp.float32)
    mean = jnp.mean(floats * floats, axis=1, keepdims=True)
    x_out[...] = (floats * lax.rsqrt(mean + EPS)).astype(jnp.bfloat16)


def columns_kernel(wq_ref, wk_ref, wv_ref, wq_out, wkv_out, w_scr, sems):
    share = wq_out.shape[0]
    window = w_scr.shape[2]
    first = peer("patch", 0) * share
    lanes = jnp.minimum(first - jnp.bitwise_and(first, 127), WIDTH - window)
    copies = []
    for i, w_ref in enumerate((wq_ref, wk_ref, wv_ref)):
        source = w_ref.at[:, pl.ds(pl.multiple_of(lanes, 128), window)]
        copies.append(pltpu.make_async_copy(source, w_scr.at[i], sems.at[i]))
        copies[-1].start()
    row = lax.broadcasted_iota(jnp.int32, (share, window), 0)
    col = lax.broadcasted_iota(jnp.int32, (share, window), 1)
    pick = (col == row + (first - lanes)).astype(jnp.float32).astype(jnp.bfloat16)
    got = []
    for i in range(3):
        copies[i].wait()
        got.append(lax.dot_general(pick, w_scr[i], NT, preferred_element_type=jnp.float32))
    wq_out[...] = got[0].astype(jnp.bfloat16)
    wkv_out[...] = jnp.concatenate(got[1:], axis=0).astype(jnp.bfloat16)


def target_kernel(owners, assign_ref, tgt_ref):
    groups = assign_ref.shape[1]
    owner = assign_ref[...]
    ids = lax.broadcasted_iota(jnp.int32, (max(owners, 8), groups), 0)
    named = (ids == owner).astype(jnp.float32)
    r = lax.broadcasted_iota(jnp.int32, (groups, groups), 0)
    c = lax.broadcasted_iota(jnp.int32, (groups, groups), 1)
    before = (r < c).astype(jnp.float32)
    seen = jnp.dot(named, before, preferred_element_type=jnp.float32)
    rank = jnp.sum(seen * named, axis=0, keepdims=True)
    token = lax.broadcasted_iota(jnp.int32, (groups, groups * APP), 1)
    group = lax.broadcasted_iota(jnp.int32, (groups, groups * APP), 0)
    mine = jnp.logical_and(token >= group * APP, token < group * APP + APP).astype(jnp.float32)
    both = jnp.concatenate(
        (
            jnp.broadcast_to(owner.astype(jnp.float32), (8, groups)),
            jnp.broadcast_to(rank, (8, groups)),
        ),
        axis=0,
    )
    tgt_ref[...] = jnp.dot(both, mine, preferred_element_type=jnp.float32).astype(jnp.bfloat16)


def stage_kernel(k0_ref, v0_ref, k1_ref, v1_ref, kk_ref, vt_ref, v_scr, sems):
    copies = [
        pltpu.make_async_copy(v0_ref, v_scr.at[0], sems.at[0]),
        pltpu.make_async_copy(v1_ref, v_scr.at[1], sems.at[1]),
        pltpu.make_async_copy(k0_ref, kk_ref.at[0], sems.at[2]),
        pltpu.make_async_copy(k1_ref, kk_ref.at[1], sems.at[3]),
    ]
    for copy in copies:
        copy.start()
    for j in range(2):
        copies[j].wait()
        for h in range(HEADS):
            lo, hi = h * HD, (h + 1) * HD
            vt_ref[j, lo:hi, :] = v_scr[j, :, lo:hi].astype(jnp.float32).T.astype(jnp.bfloat16)
    copies[2].wait()
    copies[3].wait()


def gather_weights_kernel(shards, kinds, *refs):
    w_refs, (out_ref, scr) = refs[: 2 * shards], refs[2 * shards :]
    share, depth = w_refs[0].shape[0] // kinds, w_refs[0].shape[1]
    for j in range(2):
        for s in range(shards):
            for i in range(kinds):
                rows = part(core(j) + 2 * i, share)
                piece = w_refs[j * shards + s][...].astype(jnp.float32)
                scr[rows, part(peer("stream", s), depth)] = piece[i * share : (i + 1) * share]
    out_ref[...] = scr[...].astype(jnp.bfloat16)


def project_q_kernel(chips, w_ref, tgt_ref, *refs):
    x_refs, (q_ref, x_ref) = refs[:chips], refs[chips:]
    wide = w_ref.shape[0]
    rows = x_refs[0].shape[0]
    for s in range(chips):
        x_ref[part(chip(s), rows), :] = x_refs[s][...]
    q_ref[wide:, :] = jnp.zeros_like(q_ref[wide:, :])
    q_ref[wide:, 0:rows] = tgt_ref[...]
    q_ref[0:wide, :] = lax.dot_general(
        w_ref[...], x_ref[...], NT, preferred_element_type=jnp.float32
    ).astype(jnp.bfloat16)


def slots_of(names, chips, most, source):
    both = names.astype(jnp.float32).astype(jnp.int32)
    inner = jnp.bitwise_and(lax.broadcasted_iota(jnp.int32, both[0:8].shape, 1), APP - 1)
    return (both[0:8] * chips + source) * (most * APP) + both[8:16] * APP + inner


def own_kernel(chips, most, tgt_ref, out_ref):
    out_ref[...] = slots_of(tgt_ref[...], chips, most, chip(0))


def project_kv_kernel(chips, x_ref, w_ref, kv_ref, *out_refs):
    kv_ref[...] = lax.dot_general(
        w_ref[...], x_ref[...], NT, preferred_element_type=jnp.float32
    ).astype(jnp.bfloat16)
    wide = kv_ref.shape[0] // 2
    rows = x_ref.shape[0] // chips
    for s in range(chips):
        out_refs[s][0] = kv_ref[0:wide, part(chip(s), rows)]
        out_refs[s][1] = kv_ref[wide:, part(chip(s), rows)]


def hits_kernel(chips, most, own_ref, *refs):
    q_refs, refs = refs[: chips - 1], refs[chips - 1 :]
    out_refs, (t_scr,) = refs[:chips], refs[chips:]
    slots, tokens = out_refs[0].shape
    rows = tokens // chips
    t_scr[:, part(chip(0), rows)] = own_ref[...]
    for s in range(1, chips):
        q_ref = q_refs[s - 1]
        names = q_ref[q_ref.shape[0] - 16 :, 0:rows]
        t_scr[:, part(chip(s), rows)] = slots_of(names, chips, most, chip(s))
    targets = t_scr[0:1, :]
    slot = lax.broadcasted_iota(jnp.int32, (slots, tokens), 0)
    for s in range(chips):
        hit = slot == targets - chip(s) * slots
        out_refs[s][...] = hit.astype(jnp.float32).astype(jnp.bfloat16)


def select_kernel(chips, *refs):
    hit_refs, (kv_ref, *out_refs) = refs[:chips], refs[chips:]
    wide = kv_ref.shape[0] // 2
    for s in range(chips):
        got = lax.dot_general(
            kv_ref[...], hit_refs[s][...], NT, preferred_element_type=jnp.float32
        )
        out_refs[s][0] = got[:wide].astype(jnp.bfloat16)
        out_refs[s][1] = got[wide:].astype(jnp.bfloat16)


def each_tile(count, tile, one):
    if count <= 2:
        for j in range(count):
            one(j * tile)
    else:
        lax.fori_loop(
            0, count, lambda j, c: (one(pl.multiple_of(j * tile, tile)), c)[1], 0
        )


def head_group(chips, flip):
    top = jnp.bitwise_and(chip(0), chips // 2) > 0
    return jnp.where(top, 1 - flip, flip) * (HEADS // 2)


def with_ones(value):
    return jnp.concatenate((value, jnp.ones((16, value.shape[1]), value.dtype)), axis=0)


def odd_chip():
    return jnp.bitwise_and(chip(0), 1)


def heads_of(chips, kind):
    half = HEADS // 2
    if kind < 2:
        return head_group(chips, kind), half
    if kind == 2:
        return head_group(chips, 0) + odd_chip() * (half - 1), 1
    return head_group(chips, 0) + (1 - odd_chip()), half - 1


def cached_kernel(chips, kind, tile, len0_ref, len1_ref, *refs):
    used = 1 if kind == 2 else chips // 2
    q_refs, refs = refs[:used], refs[used:]
    kk_ref, vt_ref, q_all, acc_ref, top_ref, total_ref = refs[:6]
    wide = q_refs[0].shape[0] - 16
    first, count = heads_of(chips, kind)
    if kind == 2:
        q_all[...] = q_refs[0][pl.ds(pl.multiple_of(odd_chip() * (wide - HD), wide - HD), HD), :]
    else:
        q_scr = q_all if kind < 2 else refs[6]
        for i in range(used):
            at = jnp.bitwise_and(chip(i), chips // 2 - 1)
            q_scr[part(at, wide), :] = q_refs[i][0:wide, :]
        if kind == 3:
            rest = pl.ds(pl.multiple_of((1 - odd_chip()) * HD, HD), count * HD)
            q_all[...] = q_scr[rest, :]
    tokens = q_all.shape[1]
    capacity = kk_ref.shape[1]
    short = min(2 * BLOCK, capacity)
    lengths = (len0_ref[0], len1_ref[0])

    def run(sizes):
        def head(h):
            at = part(h, HD)
            row = part(h, 8)
            keys = [kk_ref[i, 0 : sizes[i], part(first + h, HD)] for i in range(2)]
            values = [with_ones(vt_ref[i, part(first + h, HD), 0 : sizes[i]]) for i in range(2)]

            def several(j):
                lanes = [pl.ds(j + t * tile, tile) for t in range(min(2, tokens // tile))]
                scores = []
                for lane in lanes:
                    q = q_all[at, lane]
                    both = []
                    for i in range(2):
                        s = jnp.dot(keys[i], q, preferred_element_type=jnp.float32)
                        if sizes[i] == short:
                            pos = lax.broadcasted_iota(jnp.int32, s.shape, 0)
                            s = jnp.where(pos < lengths[i] * BLOCK, s, MASKED)
                        both.append(s)
                    scores.append(both)
                tops = [
                    jnp.maximum(*[jnp.max(s, axis=0, keepdims=True) for s in both])
                    for both in scores
                ]
                weights = [
                    [jnp.exp2((s - top) * EXP_SCALE).astype(jnp.bfloat16) for s in both]
                    for both, top in zip(scores, tops)
                ]
                numers = [
                    sum(
                        jnp.dot(v, w, preferred_element_type=jnp.float32)
                        for v, w in zip(values, both)
                    )
                    for both in weights
                ]
                for lane, top, numer in zip(lanes, tops, numers):
                    acc_ref[at, lane] = numer[:HD]
                    top_ref[row, lane] = jnp.broadcast_to(top, (8, tile))
                    total_ref[row, lane] = numer[HD : HD + 8]

            step = min(2 * tile, tokens)
            each_tile(tokens // step, step, several)

        if count == 1:
            head(0)
        else:
            lax.fori_loop(0, count, lambda h, c: (head(h), c)[1], 0)

    brief = [length * BLOCK <= short for length in lengths]
    if capacity <= short:
        run((short, short))
    else:
        for sizes in ((short, short), (short, capacity), (capacity, short), (capacity, capacity)):
            want = [size == short for size in sizes]
            fits = [b if w else jnp.logical_not(b) for b, w in zip(brief, want)]

            @pl.when(jnp.logical_and(*fits))
            def _(sizes=sizes):
                run(sizes)


def rows_to_levels(stat):
    stat = stat.astype(jnp.float32)
    return stat[0:8] + stat[8:16] + stat[16:24]


def dense_join_kernel(chips, *refs):
    kv_refs, out_ref = refs[:chips], refs[chips]
    for s in range(chips):
        for i in range(2):
            out_ref[i, part(chip(s), kv_refs[s].shape[1]), :] = kv_refs[s][i]


def appended_kernel(chips, kinds, tile, *refs):
    kv_refs, refs = refs[:2], refs[2:]
    states = [refs[4 * i : 4 * i + 4] for i in range(len(kinds))]
    refs = refs[4 * len(kinds) :]
    out_refs, (kt_scr, vt_scr, out_scr, level_scr) = refs[:chips], refs[chips:]
    rows = kv_refs[0].shape[2]
    for j in range(2):
        kt_scr[:, j * rows : (j + 1) * rows] = kv_refs[j][0]
        vt_scr[:, j * rows : (j + 1) * rows] = kv_refs[j][1]
    tokens = level_scr.shape[1]

    def several(j):
        lanes = pl.ds(j, tile)
        groups = [heads_of(chips, kind) for kind in kinds]
        units = [(i, h) for i, (_, count) in enumerate(groups) for h in range(count)]
        heads = [groups[i][0] + h for i, h in units]
        scores = [
            lax.dot_general(
                kt_scr[part(head, HD), :],
                states[i][0][h * HD : (h + 1) * HD, lanes],
                TN,
                preferred_element_type=jnp.float32,
            )
            for (i, h), head in zip(units, heads)
        ]
        olds = [states[i][2][8 * h : 8 * h + 1, lanes] for i, h in units]
        tops = [jnp.maximum(jnp.max(s, axis=0, keepdims=True), o) for s, o in zip(scores, olds)]
        weights = [
            jnp.exp2((s - top) * EXP_SCALE).astype(jnp.bfloat16) for s, top in zip(scores, tops)
        ]
        numers = [
            jnp.dot(with_ones(vt_scr[part(head, HD), :]), w, preferred_element_type=jnp.float32)
            for head, w in zip(heads, weights)
        ]
        row = lax.broadcasted_iota(jnp.int32, (8, tile), 0)
        levels = jnp.zeros((8, tile), jnp.float32)
        for (i, h), head, old_top, top, numer in zip(units, heads, olds, tops, numers):
            old = jnp.exp2((old_top - top) * EXP_SCALE)
            total = numer[HD : HD + 1] + states[i][3][8 * h : 8 * h + 1, lanes] * old
            inverse = 1.0 / total
            mixed = states[i][1][h * HD : (h + 1) * HD, lanes] * (old * inverse)
            mixed = mixed + numer[:HD] * inverse
            out_scr[part(head, HD), lanes] = mixed.astype(jnp.bfloat16)
            levels = jnp.where(row == head, top * EXP_SCALE + jnp.log2(total), levels)
        level_scr[:, lanes] = levels

    each_tile(tokens // tile, tile, several)
    level = level_scr[...]
    high = level.astype(jnp.bfloat16)
    rest = level - high.astype(jnp.float32)
    middle = rest.astype(jnp.bfloat16)
    low = rest - middle.astype(jnp.float32)
    stat = jnp.concatenate(
        (high.astype(jnp.float32), middle.astype(jnp.float32), low, jnp.zeros_like(low)), axis=0
    )
    out_scr[WIDTH:, :] = stat.astype(jnp.bfloat16)
    count = tokens // chips
    for s in range(chips):
        out_refs[s][...] = out_scr[:, part(chip(s), count)]


def regroup_kernel(chips, *refs):
    kv_refs, (mine_ref, other_ref) = refs[:chips], refs[chips:]
    wide, slots = kv_refs[0].shape[1], kv_refs[0].shape[2] // 2
    for s in range(chips):
        for i in range(2):
            mine_ref[i, part(chip(s), wide), :] = kv_refs[s][i, :, part(core(0), slots)]
            other_ref[i, part(chip(s), wide), :] = kv_refs[s][i, :, part(core(1), slots)]


def join_kernel(chips, mine_ref, got_ref, nk_ref, nv_ref, scr):
    size = mine_ref.shape[2] // chips
    for i, out_ref in enumerate((nk_ref, nv_ref)):
        for j, ref in enumerate((mine_ref, got_ref)):
            rows = ref[i].astype(jnp.float32).T
            for c in range(chips):
                scr[part(core(j) + 2 * c, size), :] = rows[c * size : (c + 1) * size]
        out_ref[...] = scr[...].astype(jnp.bfloat16)


def finish_kernel(count, *refs):
    got, out_ref = refs[:count], refs[count]
    levels = [rows_to_levels(got[r][WIDTH:, :]) for r in range(count)]
    best = functools.reduce(jnp.maximum, levels)
    factors = [jnp.exp2(level - best) for level in levels]
    inverse = 1.0 / functools.reduce(jnp.add, factors)
    factors = [factor * inverse for factor in factors]
    for h in range(HEADS):
        lo, hi = h * HD, (h + 1) * HD
        mixed = None
        for r in range(count):
            piece = got[r][lo:hi, :].astype(jnp.float32) * factors[r][h : h + 1, :]
            mixed = piece if mixed is None else mixed + piece
        out_ref[:, lo:hi] = mixed.T.astype(jnp.bfloat16)


def cached_kinds(owners):
    whole_head = owners // 2 == 4 and 4 * HD * 3 == 2 * WIDTH
    return (2, 3, 1) if whole_head else (0, 1)


def body(tokens, query_weight, key_weight, value_weight, cache_keys, cache_values, lengths, assign):
    owners = lax.axis_size("patch")
    shards = lax.axis_size("stream")
    chips = owners // 2
    rows, features = tokens.shape[1:]
    groups = rows // APP
    most = max(2, 2 * groups // owners)
    slots = chips * most * APP
    share = WIDTH // owners
    wide = WIDTH // chips
    half = chips * rows
    depth = query_weight.shape[0]
    cached_rows = cache_keys.shape[1]
    bf16, f32 = jnp.bfloat16, jnp.float32

    def shape(*dims, dtype=bf16):
        return jax.ShapeDtypeStruct(dims, dtype)

    def swap(x, axis, r):
        size = lax.axis_size(axis)
        return lax.ppermute(x, axis, [(i, i ^ r) for i in range(size)])

    def twin(x):
        return swap(x, "patch", 1)

    def far(parts, order=None):
        got = {0: parts[0]}
        for s in order or range(chips - 1, 0, -1):
            got[s] = swap(parts[s], "patch", 2 * s)
        return [got[s] for s in range(chips)]

    normed = call(normalize_kernel, shape(rows, features), (tokens[0],), flops=4 * rows * features)
    x_all = far([normed] * chips)
    wq, wkv = call(
        columns_kernel,
        (shape(share, depth), shape(2 * share, depth)),
        (query_weight, key_weight, value_weight),
        hbm=3,
        scratch=[pltpu.VMEM((3, depth, min(WIDTH, 256)), bf16)],
        sems=[pltpu.SemaphoreType.DMA((3,))],
        flops=6 * share * WIDTH * depth,
        limit=60 << 20,
    )
    wq_all = [wq] + [swap(wq, "stream", s) for s in range(1, shards)]
    wkv_all = [wkv] + [swap(wkv, "stream", s) for s in range(1, shards)]
    other_keys = twin(cache_keys[0])
    other_values = twin(cache_values[0])
    other_length = twin(lengths)
    tgt = call(
        functools.partial(target_kernel, owners),
        shape(16, rows),
        (assign.reshape(1, groups),),
        flops=1 << 20,
    )
    kk, vt = call(
        stage_kernel,
        (shape(2, cached_rows, WIDTH), shape(2, WIDTH, cached_rows)),
        (cache_keys[0], cache_values[0], other_keys, other_values),
        hbm=4,
        scratch=[pltpu.VMEM((2, cached_rows, WIDTH), bf16)],
        sems=[pltpu.SemaphoreType.DMA((4,))],
        flops=1 << 20,
    )

    def whole(parts, kinds):
        parts = parts + [twin(p) for p in parts]
        return call(
            functools.partial(gather_weights_kernel, shards, kinds),
            shape(kinds * wide, shards * depth),
            parts,
            scratch=[pltpu.VMEM((kinds * wide, shards * depth), f32)],
            flops=1 << 20,
        )

    wq_full = whole(wq_all, 1)
    q_own, x_full = call(
        functools.partial(project_q_kernel, chips),
        (shape(wide + 16, half), shape(half, features)),
        (wq_full, tgt, *x_all),
        flops=2 * wide * half * features,
    )
    near = list(range(1, chips // 2)) + list(range(chips // 2, chips))
    q_all = far([q_own] * chips, order=near)
    own = call(
        functools.partial(own_kernel, chips, most),
        shape(8, rows, dtype=jnp.int32),
        (tgt,),
        flops=1 << 20,
    )
    wkv_full = whole(wkv_all, 2)
    projected = call(
        functools.partial(project_kv_kernel, chips),
        (shape(2 * wide, half),) + (shape(2, wide, rows),) * chips,
        (x_full, wkv_full),
        flops=4 * wide * half * features,
    )
    kv_own, dense = projected[0], far(projected[1:])
    dense = call(
        functools.partial(dense_join_kernel, chips), shape(2, WIDTH, rows), dense, flops=1 << 20
    )
    other_dense = twin(dense)
    hits = call(
        functools.partial(hits_kernel, chips, most),
        (shape(2 * slots, half),) * chips,
        (own, *q_all[1:]),
        scratch=[pltpu.VMEM((8, half), jnp.int32)],
        flops=1 << 20,
    )
    selected = call(
        functools.partial(select_kernel, chips),
        (shape(2, wide, 2 * slots),) * chips,
        (*hits, kv_own),
        flops=8 * wide * half * slots * chips,
    )
    sent = far(selected)
    tile = min(256, half)

    def cached(kind, count):
        pieces = (q_all[: chips // 2], q_all[chips // 2 :], q_all[:1], q_all[: chips // 2])[kind]
        return call(
            functools.partial(cached_kernel, chips, kind, tile),
            (
                shape(count * HD, half),
                shape(count * HD, half, dtype=f32),
                shape(8 * count, half, dtype=f32),
                shape(8 * count, half, dtype=f32),
            ),
            (lengths[0], other_length[0], *pieces, kk, vt),
            smem=2,
            scratch=[pltpu.VMEM((WIDTH // 2, half), bf16)] if kind == 3 else [],
            flops=8 * cached_rows * half * count * HD,
        )

    kinds = cached_kinds(owners)
    counts = {0: HEADS // 2, 1: HEADS // 2, 2: 1, 3: HEADS // 2 - 1}
    states = [array for kind in kinds for array in cached(kind, counts[kind])]
    parts = call(
        functools.partial(appended_kernel, chips, kinds, min(512, half)),
        (shape(WIDTH + STAT_ROWS, rows),) * chips,
        (dense, other_dense, *states),
        scratch=[
            pltpu.VMEM((WIDTH, 2 * rows), bf16),
            pltpu.VMEM((WIDTH, 2 * rows), bf16),
            pltpu.VMEM((WIDTH + STAT_ROWS, half), bf16),
            pltpu.VMEM((8, half), f32),
        ],
        flops=8 * rows * half * WIDTH,
    )
    got = far(parts)
    mine, other = call(
        functools.partial(regroup_kernel, chips), (shape(2, WIDTH, slots),) * 2, sent, flops=1 << 20
    )
    new_keys, new_values = call(
        functools.partial(join_kernel, chips),
        (shape(2 * slots, WIDTH),) * 2,
        (mine, twin(other)),
        scratch=[pltpu.VMEM((2 * slots, WIDTH), f32)],
        flops=1 << 20,
    )
    attended = call(
        functools.partial(finish_kernel, chips),
        shape(rows, WIDTH),
        got,
        flops=4 * chips * rows * WIDTH,
    )
    return attended[None], new_keys[None], new_values[None]


def solution(mesh):
    placed = (
        P("stream", "patch", None),
        P("stream", None),
        P("stream", None),
        P("stream", None),
        P("stream", "patch", None),
        P("stream", "patch", None),
        P("stream", "patch"),
        P("stream", "patch", None),
    )
    return jax.shard_map(
        body,
        mesh=mesh,
        in_specs=placed,
        out_specs=(
            P("stream", "patch", None),
            P("stream", "patch", None),
            P("stream", "patch", None),
        ),
        check_vma=False,
    )
```
